32 devices in a mesh: hyp: 2 (over x), rows: 16 (over z, y, core).
Axes of the slice: x: 2, y: 2, z: 4, core: 2. Of those that a mesh axis runs over, the one named last changes fastest.
Arguments:
- offsets: float32 [2, 65536], P(None, 'rows'), may hold values from 0 to 1
- tile_cell: int32 [512], P('rows'), may hold values from 0 to 31, as said below
- probes: int32 [8, 65536], P(None, 'rows'), may hold values from 0 to 1
- target: float32 [65536], P('rows'), may hold values from -6 to 6
- lengthscale: float32 [2], P('hyp'), parts along dimension 0, may hold values from 0.5 to 1
- amplitude: float32 [2], P('hyp'), parts along dimension 0, may hold values from 0.02 to 0.08
- noise: float32 [2], P('hyp'), parts along dimension 0, may hold values from 0.1 to 0.4
Outputs:
- solutions: float32 [18, 65536], P('hyp', 'rows'), parts along dimension 0
- quadratic: float32 [18], P('hyp'), parts along dimension 0
The draws below stay inside these ranges and needn't reach their ends.
There are 2 independent parts, one for each index of `hyp`. The reference program is written for one: setup_inputs(seed, part) draws one part's arguments, and reference() takes and returns one part's arrays. A program takes and returns all parts, laid end to end along the dimension named above; an argument that names none is the same for every part. Nothing has to cross between parts.
Inputs may be any that keep to these rules, and one draw needn't show every extreme that they name: `tile_cell`: each aligned block of 32 entries (one device's tiles) is a permutation of 0 to 31.
All inputs are finite; a program needn't handle non-finite values.
Results may differ from the reference program's by a relative error of at most 0.0003.
Values sent between devices are 32-bit elements; how exact they have to be, the bound alone decides.
A program may use at most 64 MiB of HBM per device.

```python
import math
import jax
import jax.numpy as jnp
from jax import lax

TILE = 128
GX = 16
PROBES = 8
ITERS = 3
RHS = 9
TPD = 32
NTR = 32
NTILES = 512
NPTS = 65536


def draw_tile_cell(key, part):
    scores = jax.random.randint(jax.random.fold_in(key, 17), (NTILES // TPD, TPD), 0, 1 << 30)
    placing = jnp.argsort(scores, axis=1, stable=True)
    return placing.reshape(NTILES).astype(jnp.int32)


def set_ends(drawn, key, least, top_value):
    place = [jax.random.randint(jax.random.fold_in(key, axis), (), 0, length) for axis, length in enumerate(drawn.shape)]
    main_axis = drawn.shape.index(max(drawn.shape))
    neighbour = place[:main_axis] + [(place[main_axis] + 1) % drawn.shape[main_axis]] + place[main_axis + 1:]
    return drawn.at[tuple(place)].set(least).at[tuple(neighbour)].set(top_value)


def block_scale(key, dims, shards, low, largest):
    def one(dim, shards_of):
        draws = jax.random.uniform(jax.random.fold_in(jax.random.fold_in(key, 6), dim), (shards_of,), jnp.float32, low / len(shards), largest / len(shards))
        return jnp.repeat(jnp.exp(draws), dims[dim] // shards_of).reshape((-1,) + (1,) * (len(dims) - dim - 1))

    factor_of = one(*shards[0])
    for cut in shards[1:]:
        factor_of = factor_of * one(*cut)
    return factor_of


def scatter_about(key, extent, scale, reach, shards=(), kind=jnp.bfloat16):
    array = scale * jax.random.normal(key, extent, jnp.float32)
    if shards:
        array = array * block_scale(key, extent, shards, -0.22, 0.18)
    return jnp.clip(array, -reach, reach).astype(kind)


def setup_inputs(seed: int = 0, part: int = 0) -> dict:
    streams_of = jax.random.split(jax.random.key(seed), 8)
    part_splits = jax.random.split(jax.random.fold_in(streams_of[7], part), 8)
    offsets = jnp.clip(1.0 * jax.random.uniform(streams_of[0], (2, NPTS), jnp.float32) ** block_scale(streams_of[0], (2, NPTS), ((1, 16),), -0.2, 0.2), 0.0, 1.0)
    tile_cell = draw_tile_cell(jax.random.fold_in(streams_of[7], 71), part)
    probes = set_ends(jax.random.randint(streams_of[2], (PROBES, NPTS), 0, 2), jax.random.fold_in(streams_of[2], 1), 0, 1).astype(jnp.int32)
    target = scatter_about(streams_of[3], (NPTS,), 1.0, 6.0, ((0, 16),), jnp.float32)
    lengthscale = jnp.clip(jnp.exp(jax.random.uniform(part_splits[4], (1,), jnp.float32, math.log(0.5), math.log(1.0))), 0.5, 1.0)
    amplitude = jnp.clip(jnp.exp(jax.random.uniform(part_splits[5], (1,), jnp.float32, math.log(0.02), math.log(0.08))), 0.02, 0.08)
    noise = jnp.clip(jnp.exp(jax.random.uniform(part_splits[6], (1,), jnp.float32, math.log(0.1), math.log(0.4))), 0.1, 0.4)
    return {"offsets": offsets, "tile_cell": tile_cell, "probes": probes, "target": target, "lengthscale": lengthscale, "amplitude": amplitude, "noise": noise}


def wendland(distance):
    closeness = jnp.maximum(1.0 - distance, 0.0)
    return closeness ** 4 * (4.0 * distance + 1.0)

def kernel_sum(vectors, padded_vectors, coords, padded_coords, inverse_length, amplitude, noise):
    row_count = vectors.shape[1]
    col_count = vectors.shape[2]
    total = noise * vectors
    for row_shift in (-1, 0, 1):
        for col_shift in (-1, 0, 1):
            other = padded_coords[:, 1 + row_shift:1 + row_shift + row_count, 1 + col_shift:1 + col_shift + col_count, :]
            values = padded_vectors[:, 1 + row_shift:1 + row_shift + row_count, 1 + col_shift:1 + col_shift + col_count, :]
            delta_rows = coords[0][..., :, None] - other[0][..., None, :]
            delta_cols = coords[1][..., :, None] - other[1][..., None, :]
            distance = jnp.sqrt(delta_rows * delta_rows + delta_cols * delta_cols) * inverse_length
            weights = amplitude * wendland(distance)
            total = total + jnp.einsum('rabj,abij->rabi', values, weights, precision=lax.Precision.HIGHEST)
    return total

def to_grid(stored, order):
    lead = stored.shape[0]
    tiles = stored.reshape(lead, NTILES, TILE)[:, order]
    return tiles.reshape(lead, NTR, GX, TILE)

def reference(offsets, tile_cell, probes, target, lengthscale, amplitude, noise):
    device_base = jnp.arange(NTILES, dtype=jnp.int32) // TPD * TPD
    cell = (tile_cell + device_base).astype(jnp.int32)
    order = jnp.argsort(cell).astype(jnp.int32)
    grid_offsets = to_grid(offsets, order)
    row_place = jnp.arange(NTR, dtype=jnp.float32)[:, None, None]
    col_place = jnp.arange(GX, dtype=jnp.float32)[None, :, None]
    coords = jnp.stack([grid_offsets[0] + row_place, grid_offsets[1] + col_place])
    padded_coords = jnp.pad(coords, ((0, 0), (1, 1), (1, 1), (0, 0)))
    signs = 2.0 * probes.astype(jnp.float32) - 1.0
    right_sides = to_grid(jnp.concatenate([signs, target[None, :]], axis=0), order)
    inverse_length = 1.0 / lengthscale[0]

    def operate(vectors):
        padded = jnp.pad(vectors, ((0, 0), (1, 1), (1, 1), (0, 0)))
        return kernel_sum(vectors, padded, coords, padded_coords, inverse_length, amplitude[0], noise[0])

    def widen(scalars):
        return scalars[:, None, None, None]
    iterate = jnp.zeros_like(right_sides)
    residual = right_sides
    direction = right_sides
    norm_now = lax.optimization_barrier(jnp.sum(residual * residual, axis=(1, 2, 3)))
    for iteration in range(ITERS):
        image = operate(direction)
        alpha = norm_now / lax.optimization_barrier(jnp.sum(direction * image, axis=(1, 2, 3)))
        iterate = iterate + widen(alpha) * direction
        residual = residual - widen(alpha) * image
        if iteration + 1 < ITERS:
            norm_next = lax.optimization_barrier(jnp.sum(residual * residual, axis=(1, 2, 3)))
            direction = residual + widen(norm_next / norm_now) * direction
            norm_now = norm_next
    quadratic = lax.optimization_barrier(jnp.sum(right_sides * iterate, axis=(1, 2, 3))) / NPTS
    solutions = iterate.reshape(RHS, NTILES, TILE)[:, cell].reshape(RHS, NPTS)
    return (solutions, quadratic)
```

```python
import functools

import jax
import jax.numpy as jnp
from jax import lax
from jax.experimental import pallas as pl
from jax.experimental.pallas import tpu as pltpu
from jax.sharding import PartitionSpec as P

TILE = 128
GX = 16
RHS = 9
PAD = 16
FAR = 1.0e3
TINY = 1.0e-30
MESH = pl.DeviceIdType.MESH
F32 = jnp.float32
BF16 = jnp.bfloat16


def kernel(
    n, rows, points,
    order, cell, length, amp_ref, noise_ref, off, probes, target,
    x_ref, q_ref,
    tiles, pk, hv, vx, whi, wlo, sc, cm, acc, mom, gathered,
    halo_send, halo_recv, mom_send, mom_recv,
):
    me = lax.axis_index("rows")
    has = (me > 0, me < n - 1)
    row_lanes = GX * TILE
    reach = 3 * TILE
    amp = amp_ref[0]
    shift = amp + noise_ref[0]

    barrier = pltpu.get_barrier_semaphore()

    def greet(k, carry):
        pl.semaphore_signal(
            barrier, inc=1, device_id={"rows": lax.rem(me + k, n)}, device_id_type=MESH
        )
        return carry

    lax.fori_loop(1, n, greet, 0)

    for g in range(rows * GX):
        lanes = slice(g * TILE, (g + 1) * TILE)
        tiles[g] = jnp.concatenate(
            [
                2.0 * probes[:, lanes].astype(F32) - 1.0,
                target[:, lanes],
                off[:, lanes],
                jnp.zeros((PAD - RHS - 2, TILE), F32),
            ],
            axis=0,
        )
    for g in range(rows * GX):
        pk[0, :, g * TILE : (g + 1) * TILE] = tiles[order[g]]

    pl.semaphore_wait(barrier, n - 1)

    def halo_copy(k, side):
        first = 0 if side == 0 else (rows - 1) * row_lanes
        return pltpu.make_async_remote_copy(
            src_ref=pk.at[k, :, pl.ds(first, row_lanes)],
            dst_ref=hv.at[k, 1 - side],
            send_sem=halo_send.at[k, side],
            recv_sem=halo_recv.at[k, 1 - side],
            device_id={"rows": me - 1 if side == 0 else me + 1},
            device_id_type=MESH,
        )

    def send_halo(k):
        for side in range(2):
            @pl.when(has[side])
            def _(side=side):
                halo_copy(k, side).start()

    send_halo(0)

    inverse = 1.0 / jnp.full((1, TILE), length[0], F32)

    def place_columns(sr, values):
        cm[0:GX] = jnp.concatenate([v[0] for v in values], axis=0)
        cm[GX : 2 * GX] = jnp.concatenate([v[1] for v in values], axis=0)
        turned = cm[...].T
        for c in range(GX):
            at = slice((c + 1) * TILE, (c + 2) * TILE)
            sc[0, sr, at, :] = jnp.broadcast_to(turned[:, c : c + 1], (TILE, TILE))
            sc[1, sr, at, :] = jnp.broadcast_to(turned[:, GX + c : GX + c + 1], (TILE, TILE))

    vx[...] = jnp.zeros_like(vx)
    cm[...] = jnp.zeros_like(cm)
    for sr in range(rows + 2):
        for edge in (0, (GX + 1) * TILE):
            sc[0, sr, edge : edge + TILE, :] = jnp.full((TILE, TILE), FAR, F32)
            sc[1, sr, edge : edge + TILE, :] = jnp.full((TILE, TILE), FAR, F32)
    for side, sr in ((0, 0), (1, rows + 1)):
        @pl.when(jnp.logical_not(has[side]))
        def _(sr=sr):
            sc[0, sr] = jnp.full((sc.shape[2], TILE), FAR, F32)
            sc[1, sr] = jnp.full((sc.shape[2], TILE), FAR, F32)

    def split(par, sr, at, value):
        high = value.astype(BF16)
        vx[par, sr, 0:PAD, at] = high
        vx[par, sr, PAD : 2 * PAD, at] = (value - high.astype(F32)).astype(BF16)

    own = pl.ds(TILE, row_lanes)
    for a in range(rows):
        base = a * row_lanes
        split(0, a + 1, own, pk[0, :, base : base + row_lanes])
        place_columns(
            a + 1,
            [
                (
                    (pk[0, RHS : RHS + 1, base + c * TILE : base + (c + 1) * TILE] + a) * inverse,
                    (pk[0, RHS + 1 : RHS + 2, base + c * TILE : base + (c + 1) * TILE] + c) * inverse,
                )
                for c in range(GX)
            ],
        )

    def build(a, c, srs):
        base = pl.multiple_of(a * row_lanes + c * TILE, TILE)
        here = pk[0, :, pl.ds(base, TILE)]
        tx = (here[RHS : RHS + 1] + a) * inverse
        ty = (here[RHS + 1 : RHS + 2] + c.astype(F32)) * inverse
        step = 64
        for sr in srs:
            for part in range(reach // step):
                at = pl.ds(pl.multiple_of(c * TILE + part * step, step), step)
                dx = sc[0, sr, at, :] - tx
                dy = sc[1, sr, at, :] - ty
                square = dx * dx + dy * dy
                close = jnp.maximum(1.0 - square * lax.rsqrt(jnp.maximum(square, TINY)), 0.0)
                twice = close * close
                w = twice * twice * (5.0 - 4.0 * close)
                high = w.astype(BF16)
                to = pl.ds((sr - a) * reach + part * step, step)
                whi[a, c, to, :] = high
                wlo[a, c, to, :] = (w - high.astype(F32)).astype(BF16)

    def dots(par, a, c, srs):
        lanes = pl.ds(pl.multiple_of(c * TILE, TILE), reach)
        v = jnp.concatenate([vx[par, sr, :, lanes] for sr in srs], axis=1)
        at = pl.ds((srs[0] - a) * reach, len(srs) * reach)
        r = jnp.dot(v, whi[a, c, at, :], preferred_element_type=F32)
        s = jnp.dot(v[:PAD], wlo[a, c, at, :], preferred_element_type=F32)
        return r[:PAD] + r[PAD:] + s

    def inner_rows(a):
        return [sr for sr in range(a, a + 3) if 1 <= sr <= rows]

    def outer_rows(a):
        return [sr for sr in range(a, a + 3) if sr < 1 or sr > rows]

    zero = jnp.zeros((PAD, TILE), F32)
    moments = []
    for k in range(3):
        par = k % 2

        def inner(c, carry, k=k, par=par):
            for a in range(rows):
                if k == 0:
                    build(a, c, inner_rows(a))
                at = pl.ds(pl.multiple_of(a * row_lanes + c * TILE, TILE), TILE)
                acc[:, at] = dots(par, a, c, inner_rows(a))
            return carry

        lax.fori_loop(0, GX, inner, 0)

        for side, sr in ((0, 0), (1, rows + 1)):
            @pl.when(has[side])
            def _(side=side, sr=sr, k=k, par=par):
                pltpu.make_async_remote_copy(
                    src_ref=pk.at[k, :, pl.ds(0, row_lanes)],
                    dst_ref=hv.at[k, side],
                    send_sem=halo_send.at[k, side],
                    recv_sem=halo_recv.at[k, side],
                    device_id={"rows": me - 1 if side == 0 else me + 1},
                    device_id_type=MESH,
                ).wait_recv()
                split(par, sr, own, hv[k, side])
                if k == 0:
                    place_columns(
                        sr,
                        [
                            (
                                (hv[0, side, RHS : RHS + 1, c * TILE : (c + 1) * TILE] + (sr - 1)) * inverse,
                                (hv[0, side, RHS + 1 : RHS + 2, c * TILE : (c + 1) * TILE] + c) * inverse,
                            )
                            for c in range(GX)
                        ],
                    )

        def outer(c, carry, k=k, par=par):
            first, cross, square = carry
            for a in range(rows):
                at = pl.ds(pl.multiple_of(a * row_lanes + c * TILE, TILE), TILE)
                total = acc[:, at]
                for sr in outer_rows(a):
                    if k == 0:
                        build(a, c, [sr])
                    total = total + dots(par, a, c, [sr])
                now = pk[k, :, at]
                later = amp * (total - now)
                if k == 0:
                    first = first + now * now
                cross = cross + now * later
                if k < 2:
                    square = square + later * later
                    pk[k + 1, :, at] = later
                    split(1 - par, a + 1, pl.ds(pl.multiple_of((c + 1) * TILE, TILE), TILE), later)
            return first, cross, square

        first, cross, square = lax.fori_loop(0, GX, outer, (zero, zero, zero))
        moments += ([first] if k == 0 else []) + [cross] + ([square] if k < 2 else [])
        if k < 2:
            send_halo(k + 1)

    lane = lax.broadcasted_iota(jnp.int32, (PAD, TILE), 1)
    packed = zero
    for i, part in enumerate(moments):
        packed = jnp.where(lane == i, jnp.sum(part, axis=1, keepdims=True), packed)
    mom[...] = packed
    gathered[me] = packed

    def mom_copy(k):
        peer = lax.rem(me + k, n)
        return pltpu.make_async_remote_copy(
            src_ref=mom,
            dst_ref=gathered.at[me],
            send_sem=mom_send.at[peer],
            recv_sem=mom_recv.at[me],
            device_id={"rows": peer},
            device_id_type=MESH,
        )

    def mom_start(k, carry):
        mom_copy(k).start()
        return carry

    lax.fori_loop(1, n, mom_start, 0)

    def mom_wait(k, carry):
        peer = lax.rem(me + k, n)
        pltpu.make_async_remote_copy(
            src_ref=mom,
            dst_ref=gathered.at[peer],
            send_sem=mom_send.at[peer],
            recv_sem=mom_recv.at[peer],
            device_id={"rows": peer},
            device_id_type=MESH,
        ).wait()
        return carry

    lax.fori_loop(1, n, mom_wait, 0)
    total = lax.fori_loop(0, n, lambda j, t: t + gathered[j], zero)

    m = [total[:, i : i + 1] for i in range(6)]
    a00, a01, a02 = (m[i + 1] + shift * m[i] for i in range(3))
    a11, a12 = (m[i + 1] + shift * m[i] for i in range(2, 4))
    a22 = m[5] + shift * m[4]
    l1 = a01 / a00
    l2 = a02 / a00
    b11 = a11 - l1 * a01
    b12 = a12 - l1 * a02
    b22 = a22 - l2 * a02
    g1 = m[1] - l1 * m[0]
    g2 = m[2] - l2 * m[0]
    fine1 = b11 > 1.0e-6 * a11
    safe1 = jnp.where(fine1, b11, 1.0)
    l3 = b12 / safe1
    d22 = b22 - l3 * b12
    fine2 = jnp.logical_and(fine1, d22 > 1.0e-6 * a22)
    c2 = jnp.where(fine2, (g2 - l3 * g1) / jnp.where(fine2, d22, 1.0), 0.0)
    c1 = jnp.where(fine1, (g1 - b12 * c2) / safe1, 0.0)
    c0 = (m[0] - a01 * c1 - a02 * c2) / a00
    q_ref[...] = jnp.broadcast_to((c0 * m[0] + c1 * m[1] + c2 * m[2]) / points, (PAD, TILE))

    for g in range(rows * GX):
        at = slice(g * TILE, (g + 1) * TILE)
        tiles[g] = c0 * pk[0, :, at] + c1 * pk[1, :, at] + c2 * pk[2, :, at]
    for s in range(rows * GX):
        found = tiles[cell[s]]
        x_ref[:, s * TILE : (s + 1) * TILE] = found[:RHS]

    for k in range(3):
        for side in range(2):
            @pl.when(has[side])
            def _(k=k, side=side):
                halo_copy(k, side).wait_send()


def shards(n, offsets, tile_cell, probes, target, lengthscale, amplitude, noise):
    tiles = tile_cell.shape[0]
    rows = tiles // GX
    places = jnp.arange(tiles, dtype=jnp.int32)
    order = jnp.sum(
        jnp.where(tile_cell[None, :] == places[:, None], places[None, :], 0), axis=1
    ).astype(jnp.int32)
    local = tiles * TILE
    width = (GX + 2) * TILE
    smem = pl.BlockSpec(memory_space=pltpu.SMEM)
    vmem = pl.BlockSpec(memory_space=pltpu.VMEM)
    solutions, quadratic = pl.pallas_call(
        functools.partial(kernel, n, rows, float(local * n)),
        out_shape=(
            jax.ShapeDtypeStruct((RHS, local), F32),
            jax.ShapeDtypeStruct((PAD, TILE), F32),
        ),
        in_specs=[smem] * 5 + [vmem] * 3,
        out_specs=(vmem, vmem),
        scratch_shapes=[
            pltpu.VMEM((tiles, PAD, TILE), F32),
            pltpu.VMEM((3, PAD, local), F32),
            pltpu.VMEM((3, 2, PAD, GX * TILE), F32),
            pltpu.VMEM((2, rows + 2, 2 * PAD, width), BF16),
            pltpu.VMEM((rows, GX, 9 * TILE, TILE), BF16),
            pltpu.VMEM((rows, GX, 9 * TILE, TILE), BF16),
            pltpu.VMEM((2, rows + 2, width, TILE), F32),
            pltpu.VMEM((TILE, TILE), F32),
            pltpu.VMEM((PAD, local), F32),
            pltpu.VMEM((PAD, TILE), F32),
            pltpu.VMEM((n, PAD, TILE), F32),
            pltpu.SemaphoreType.DMA((3, 2)),
            pltpu.SemaphoreType.DMA((3, 2)),
            pltpu.SemaphoreType.DMA((n,)),
            pltpu.SemaphoreType.DMA((n,)),
        ],
        compiler_params=pltpu.CompilerParams(
            collective_id=0, has_side_effects=True, vmem_limit_bytes=58 * 1024 * 1024
        ),
        name="solve",
    )(order, tile_cell, lengthscale, amplitude, noise, offsets, probes, target[None, :])
    return solutions, quadratic[:RHS, 0]


def solution(mesh):
    return jax.shard_map(
        functools.partial(shards, mesh.shape["rows"]),
        mesh=mesh,
        in_specs=(
            P(None, "rows"),
            P("rows"),
            P(None, "rows"),
            P("rows"),
            P("hyp"),
            P("hyp"),
            P("hyp"),
        ),
        out_specs=(P("hyp", "rows"), P("hyp")),
        check_vma=False,
    )
```

```python
import functools

import jax
import jax.numpy as jnp
from jax import lax
from jax.experimental import pallas as pl
from jax.experimental.pallas import tpu as pltpu
from jax.sharding import PartitionSpec as P

TILE = 128
GX = 16
RHS = 9
PAD = 16
FAR = 1.0e3
TINY = 1.0e-30
MESH = pl.DeviceIdType.MESH
F32 = jnp.float32
BF16 = jnp.bfloat16


def kernel(
    n, rows, points,
    order, cell, length, amp_ref, noise_ref, off_in, probes_in, target_in,
    x_ref, q_ref,
    off, probes, target, tiles, pk, hv, vx, whi, wlo, ohi, olo, sc, cm, acc, mom, gathered,
    load_sem, halo_send, halo_recv, mom_send, mom_recv,
):
    me = lax.axis_index("rows")
    has = (me > 0, me < n - 1)
    row_lanes = GX * TILE
    reach = 3 * TILE
    amp = amp_ref[0]
    shift = amp + noise_ref[0]

    barrier = pltpu.get_barrier_semaphore()

    def greet(k, carry):
        pl.semaphore_signal(
            barrier, inc=1, device_id={"rows": lax.rem(me + k, n)}, device_id_type=MESH
        )
        return carry

    lax.fori_loop(1, n, greet, 0)
    loads = [
        pltpu.make_async_copy(source, held, load_sem.at[i])
        for i, (source, held) in enumerate(
            ((off_in, off), (probes_in, probes), (target_in, target))
        )
    ]
    for load in loads:
        load.start()
    vx[...] = jnp.zeros_like(vx)
    cm[...] = jnp.zeros_like(cm)
    for sr in range(rows + 2):
        for edge in (0, (GX + 1) * TILE):
            sc[0, sr, edge : edge + TILE, :] = jnp.full((TILE, TILE), FAR, F32)
            sc[1, sr, edge : edge + TILE, :] = jnp.full((TILE, TILE), FAR, F32)
    for load in loads:
        load.wait()

    for g in range(rows * GX):
        lanes = slice(g * TILE, (g + 1) * TILE)
        tiles[g] = jnp.concatenate(
            [
                2.0 * probes[:, lanes].astype(F32) - 1.0,
                target[:, lanes],
                off[:, lanes],
                jnp.zeros((PAD - RHS - 2, TILE), F32),
            ],
            axis=0,
        )
    for g in range(rows * GX):
        pk[0, :, g * TILE : (g + 1) * TILE] = tiles[order[g]]

    pl.semaphore_wait(barrier, n - 1)

    def halo_copy(k, side):
        first = 0 if side == 0 else (rows - 1) * row_lanes
        return pltpu.make_async_remote_copy(
            src_ref=pk.at[k, :, pl.ds(first, row_lanes)],
            dst_ref=hv.at[k, 1 - side],
            send_sem=halo_send.at[k, side],
            recv_sem=halo_recv.at[k, 1 - side],
            device_id={"rows": me - 1 if side == 0 else me + 1},
            device_id_type=MESH,
        )

    def send_halo(k):
        for side in range(2):
            @pl.when(has[side])
            def _(side=side):
                halo_copy(k, side).start()

    send_halo(0)

    inverse = 1.0 / jnp.full((1, TILE), length[0], F32)

    def place_columns(sr, values):
        cm[0:GX] = jnp.concatenate([v[0] for v in values], axis=0)
        cm[GX : 2 * GX] = jnp.concatenate([v[1] for v in values], axis=0)
        turned = cm[...].T
        for c in range(GX):
            at = slice((c + 1) * TILE, (c + 2) * TILE)
            sc[0, sr, at, :] = jnp.broadcast_to(turned[:, c : c + 1], (TILE, TILE))
            sc[1, sr, at, :] = jnp.broadcast_to(turned[:, GX + c : GX + c + 1], (TILE, TILE))

    for side, sr in ((0, 0), (1, rows + 1)):
        @pl.when(jnp.logical_not(has[side]))
        def _(sr=sr):
            sc[0, sr] = jnp.full((sc.shape[2], TILE), FAR, F32)
            sc[1, sr] = jnp.full((sc.shape[2], TILE), FAR, F32)

    def split(par, sr, at, value):
        high = value.astype(BF16)
        vx[par, sr, 0:PAD, at] = high
        vx[par, sr, PAD : 2 * PAD, at] = (value - high.astype(F32)).astype(BF16)

    own = pl.ds(TILE, row_lanes)
    for a in range(rows):
        base = a * row_lanes
        split(0, a + 1, own, pk[0, :, base : base + row_lanes])
        place_columns(
            a + 1,
            [
                (
                    (pk[0, RHS : RHS + 1, base + c * TILE : base + (c + 1) * TILE] + a) * inverse,
                    (pk[0, RHS + 1 : RHS + 2, base + c * TILE : base + (c + 1) * TILE] + c) * inverse,
                )
                for c in range(GX)
            ],
        )

    def build(high_ref, low_ref, a, c, sr, first, lanes):
        base = pl.multiple_of(a * row_lanes + c * TILE, TILE)
        here = pk[0, :, pl.ds(base, TILE)]
        tx = (here[RHS : RHS + 1] + a) * inverse
        ty = (here[RHS + 1 : RHS + 2] + c.astype(F32)) * inverse
        step = 64
        for part in range(reach // step):
            at = pl.ds(pl.multiple_of(c * TILE + part * step, step), step)
            dx = sc[0, sr, at, :] - tx
            dy = sc[1, sr, at, :] - ty
            square = dx * dx + dy * dy
            close = jnp.maximum(1.0 - square * lax.rsqrt(jnp.maximum(square, TINY)), 0.0)
            twice = close * close
            w = twice * twice * (5.0 - 4.0 * close)
            high = w.astype(BF16)
            to = pl.ds(first + part * step, step)
            high_ref[to, lanes] = high
            low_ref[to, lanes] = (w - high.astype(F32)).astype(BF16)

    def apply(v, high_ref, low_ref):
        r = jnp.dot(v, high_ref[...], preferred_element_type=F32)
        s = jnp.dot(v[:PAD], low_ref[...], preferred_element_type=F32)
        return r[:PAD] + r[PAD:] + s

    pair = 2 * TILE
    zero = jnp.zeros((PAD, TILE), F32)
    moments = []
    for k in range(3):
        par = k % 2

        def inner(c, carry, k=k, par=par):
            if k == 0:
                for sr in range(1, rows + 1):
                    for a in range(rows):
                        build(
                            whi.at[c], wlo.at[c], a, c, sr, (sr - 1) * reach,
                            slice(a * TILE, (a + 1) * TILE),
                        )
            lanes = pl.ds(pl.multiple_of(c * TILE, TILE), reach)
            v = jnp.concatenate([vx[par, sr, :, lanes] for sr in range(1, rows + 1)], axis=1)
            part = apply(v, whi.at[c], wlo.at[c])
            for a in range(rows):
                at = pl.ds(pl.multiple_of(a * row_lanes + c * TILE, TILE), TILE)
                acc[:, at] = part[:, a * TILE : (a + 1) * TILE]
            return carry

        lax.fori_loop(0, GX, inner, 0)

        for side, sr in ((0, 0), (1, rows + 1)):
            @pl.when(has[side])
            def _(side=side, sr=sr, k=k, par=par):
                pltpu.make_async_remote_copy(
                    src_ref=pk.at[k, :, pl.ds(0, row_lanes)],
                    dst_ref=hv.at[k, side],
                    send_sem=halo_send.at[k, side],
                    recv_sem=halo_recv.at[k, side],
                    device_id={"rows": me - 1 if side == 0 else me + 1},
                    device_id_type=MESH,
                ).wait_recv()
                split(par, sr, own, hv[k, side])
                if k == 0:
                    place_columns(
                        sr,
                        [
                            (
                                (hv[0, side, RHS : RHS + 1, c * TILE : (c + 1) * TILE] + (sr - 1)) * inverse,
                                (hv[0, side, RHS + 1 : RHS + 2, c * TILE : (c + 1) * TILE] + c) * inverse,
                            )
                            for c in range(GX)
                        ],
                    )

        def outer(c, carry, k=k, par=par):
            first, cross, square = carry
            sources = pl.ds(pl.multiple_of(c * pair, pair), 2 * pair)
            for a in range(rows):
                at = pl.ds(pl.multiple_of(a * row_lanes + c * pair, pair), pair)
                total = acc[:, at]
                for side, sr, edge in ((0, 0, 0), (1, rows + 1, rows - 1)):
                    if a != edge:
                        continue
                    if k == 0:
                        for held in (ohi, olo):
                            held[side, c, 3 * TILE :, :TILE] = jnp.zeros((TILE, TILE), BF16)
                            held[side, c, :TILE, TILE:] = jnp.zeros((TILE, TILE), BF16)
                        for t in range(2):
                            build(
                                ohi.at[side, c], olo.at[side, c], a, 2 * c + t, sr, t * TILE,
                                slice(t * TILE, (t + 1) * TILE),
                            )
                    total = total + apply(
                        vx[par, sr, :, sources], ohi.at[side, c], olo.at[side, c]
                    )
                now = pk[k, :, at]
                later = amp * (total - now)
                if k == 0:
                    first = first + now * now
                cross = cross + now * later
                if k < 2:
                    square = square + later * later
                    pk[k + 1, :, at] = later
                    split(1 - par, a + 1, pl.ds(pl.multiple_of(c * pair + TILE, TILE), pair), later)
            return first, cross, square

        wide = jnp.zeros((PAD, pair), F32)
        first, cross, square = lax.fori_loop(0, GX // 2, outer, (wide, wide, wide))
        moments += ([first] if k == 0 else []) + [cross] + ([square] if k < 2 else [])
        if k < 2:
            send_halo(k + 1)

    lane = lax.broadcasted_iota(jnp.int32, (PAD, TILE), 1)
    packed = zero
    for i, part in enumerate(moments):
        packed = jnp.where(lane == i, jnp.sum(part, axis=1, keepdims=True), packed)
    mom[...] = packed
    gathered[me] = packed

    def mom_copy(k):
        peer = lax.rem(me + k, n)
        return pltpu.make_async_remote_copy(
            src_ref=mom,
            dst_ref=gathered.at[me],
            send_sem=mom_send.at[peer],
            recv_sem=mom_recv.at[me],
            device_id={"rows": peer},
            device_id_type=MESH,
        )

    def mom_start(k, carry):
        mom_copy(k).start()
        return carry

    lax.fori_loop(1, n, mom_start, 0)

    def mom_wait(k, carry):
        peer = lax.rem(me + k, n)
        pltpu.make_async_remote_copy(
            src_ref=mom,
            dst_ref=gathered.at[peer],
            send_sem=mom_send.at[peer],
            recv_sem=mom_recv.at[peer],
            device_id={"rows": peer},
            device_id_type=MESH,
        ).wait()
        return carry

    lax.fori_loop(1, n, mom_wait, 0)
    total = lax.fori_loop(0, n, lambda j, t: t + gathered[j], zero)

    m = [total[:, i : i + 1] for i in range(6)]
    a00, a01, a02 = (m[i + 1] + shift * m[i] for i in range(3))
    a11, a12 = (m[i + 1] + shift * m[i] for i in range(2, 4))
    a22 = m[5] + shift * m[4]
    l1 = a01 / a00
    l2 = a02 / a00
    b11 = a11 - l1 * a01
    b12 = a12 - l1 * a02
    b22 = a22 - l2 * a02
    g1 = m[1] - l1 * m[0]
    g2 = m[2] - l2 * m[0]
    fine1 = b11 > 1.0e-6 * a11
    safe1 = jnp.where(fine1, b11, 1.0)
    l3 = b12 / safe1
    d22 = b22 - l3 * b12
    fine2 = jnp.logical_and(fine1, d22 > 1.0e-6 * a22)
    c2 = jnp.where(fine2, (g2 - l3 * g1) / jnp.where(fine2, d22, 1.0), 0.0)
    c1 = jnp.where(fine1, (g1 - b12 * c2) / safe1, 0.0)
    c0 = (m[0] - a01 * c1 - a02 * c2) / a00
    values = (c0 * m[0] + c1 * m[1] + c2 * m[2]) / points
    sublane = lax.broadcasted_iota(jnp.int32, (PAD, TILE), 0)
    turned = jnp.sum(jnp.where(lane == sublane, values, 0.0), axis=0, keepdims=True)
    q_ref[...] = turned[:, :RHS]

    for g in range(rows * GX):
        at = slice(g * TILE, (g + 1) * TILE)
        tiles[g] = c0 * pk[0, :, at] + c1 * pk[1, :, at] + c2 * pk[2, :, at]
    for s in range(rows * GX):
        found = tiles[cell[s]]
        x_ref[:, s * TILE : (s + 1) * TILE] = found[:RHS]

    for k in range(3):
        for side in range(2):
            @pl.when(has[side])
            def _(k=k, side=side):
                halo_copy(k, side).wait_send()


def shards(n, offsets, tile_cell, probes, target, lengthscale, amplitude, noise):
    tiles = tile_cell.shape[0]
    rows = tiles // GX
    places = jnp.arange(tiles, dtype=jnp.int32)
    order = jnp.sum(
        jnp.where(tile_cell[None, :] == places[:, None], places[None, :], 0), axis=1
    ).astype(jnp.int32)
    local = tiles * TILE
    width = (GX + 2) * TILE
    smem = pl.BlockSpec(memory_space=pltpu.SMEM)
    vmem = pl.BlockSpec(memory_space=pltpu.VMEM)
    solutions, quadratic = pl.pallas_call(
        functools.partial(kernel, n, rows, float(local * n)),
        out_shape=(
            jax.ShapeDtypeStruct((RHS, local), F32),
            jax.ShapeDtypeStruct((1, RHS), F32),
        ),
        in_specs=[smem] * 5 + [pl.BlockSpec(memory_space=pl.ANY)] * 3,
        out_specs=(vmem, vmem),
        scratch_shapes=[
            pltpu.VMEM((2, local), F32),
            pltpu.VMEM((RHS - 1, local), jnp.int32),
            pltpu.VMEM((1, local), F32),
            pltpu.VMEM((tiles, PAD, TILE), F32),
            pltpu.VMEM((3, PAD, local), F32),
            pltpu.VMEM((3, 2, PAD, GX * TILE), F32),
            pltpu.VMEM((2, rows + 2, 2 * PAD, width), BF16),
            pltpu.VMEM((GX, rows * 3 * TILE, rows * TILE), BF16),
            pltpu.VMEM((GX, rows * 3 * TILE, rows * TILE), BF16),
            pltpu.VMEM((2, GX // 2, 4 * TILE, 2 * TILE), BF16),
            pltpu.VMEM((2, GX // 2, 4 * TILE, 2 * TILE), BF16),
            pltpu.VMEM((2, rows + 2, width, TILE), F32),
            pltpu.VMEM((TILE, TILE), F32),
            pltpu.VMEM((PAD, local), F32),
            pltpu.VMEM((PAD, TILE), F32),
            pltpu.VMEM((n, PAD, TILE), F32),
            pltpu.SemaphoreType.DMA((3,)),
            pltpu.SemaphoreType.DMA((3, 2)),
            pltpu.SemaphoreType.DMA((3, 2)),
            pltpu.SemaphoreType.DMA((n,)),
            pltpu.SemaphoreType.DMA((n,)),
        ],
        compiler_params=pltpu.CompilerParams(
            collective_id=0, has_side_effects=True, vmem_limit_bytes=58 * 1024 * 1024
        ),
        name="solve",
    )(order, tile_cell, lengthscale, amplitude, noise, offsets, probes, target[None, :])
    return solutions, quadratic.reshape(RHS)


def solution(mesh):
    return jax.shard_map(
        functools.partial(shards, mesh.shape["rows"]),
        mesh=mesh,
        in_specs=(
            P(None, "rows"),
            P("rows"),
            P(None, "rows"),
            P("rows"),
            P("hyp"),
            P("hyp"),
            P("hyp"),
        ),
        out_specs=(P("hyp", "rows"), P("hyp")),
        check_vma=False,
    )
```

```python
import functools

import jax
import jax.numpy as jnp
from jax import lax
from jax.experimental import pallas as pl
from jax.experimental.pallas import tpu as pltpu
from jax.sharding import PartitionSpec as P

TILE = 128
GX = 16
RHS = 9
PAD = 16
FAR = 1.0e3
TINY = 1.0e-30
MESH = pl.DeviceIdType.MESH
F32 = jnp.float32
BF16 = jnp.bfloat16


def kernel(
    n, rows, points,
    order, cell, length, amp_ref, noise_ref, off_in, probes_in, target_in,
    x_ref, q_ref,
    off, probes, target, tiles, pk, hv, vx, whi, wlo, ohi, olo, sc, cm, acc, mom, gathered,
    load_sem, halo_send, halo_recv, mom_send, mom_recv,
):
    me = lax.axis_index("rows")
    has = (me > 0, me < n - 1)
    row_lanes = GX * TILE
    reach = 3 * TILE
    amp = amp_ref[0]
    shift = amp + noise_ref[0]

    barrier = pltpu.get_barrier_semaphore()

    def greet(k, carry):
        pl.semaphore_signal(
            barrier, inc=1, device_id={"rows": lax.rem(me + k, n)}, device_id_type=MESH
        )
        return carry

    lax.fori_loop(1, n, greet, 0)
    loads = [
        pltpu.make_async_copy(source, held, load_sem.at[i])
        for i, (source, held) in enumerate(
            ((off_in, off), (probes_in, probes), (target_in, target))
        )
    ]
    for load in loads:
        load.start()
    vx[...] = jnp.zeros_like(vx)
    cm[...] = jnp.zeros_like(cm)
    for sr in range(rows + 2):
        for edge in (0, (GX + 1) * TILE):
            sc[0, sr, edge : edge + TILE, :] = jnp.full((TILE, TILE), FAR, F32)
            sc[1, sr, edge : edge + TILE, :] = jnp.full((TILE, TILE), FAR, F32)
    for load in loads:
        load.wait()

    for g in range(rows * GX):
        lanes = slice(g * TILE, (g + 1) * TILE)
        tiles[g] = jnp.concatenate(
            [
                2.0 * probes[:, lanes].astype(F32) - 1.0,
                target[:, lanes],
                off[:, lanes],
                jnp.zeros((PAD - RHS - 2, TILE), F32),
            ],
            axis=0,
        )
    for g in range(rows * GX):
        pk[0, :, g * TILE : (g + 1) * TILE] = tiles[order[g]]

    pl.semaphore_wait(barrier, n - 1)

    def halo_copy(k, side):
        first = 0 if side == 0 else (rows - 1) * row_lanes
        return pltpu.make_async_remote_copy(
            src_ref=pk.at[k, :, pl.ds(first, row_lanes)],
            dst_ref=hv.at[k, 1 - side],
            send_sem=halo_send.at[k, side],
            recv_sem=halo_recv.at[k, 1 - side],
            device_id={"rows": me - 1 if side == 0 else me + 1},
            device_id_type=MESH,
        )

    def send_halo(k):
        for side in range(2):
            @pl.when(has[side])
            def _(side=side):
                halo_copy(k, side).start()

    send_halo(0)

    inverse = 1.0 / jnp.full((1, TILE), length[0], F32)

    def place_columns(sr, values):
        cm[0:GX] = jnp.concatenate([v[0] for v in values], axis=0)
        cm[GX : 2 * GX] = jnp.concatenate([v[1] for v in values], axis=0)
        turned = cm[...].T
        for c in range(GX):
            at = slice((c + 1) * TILE, (c + 2) * TILE)
            sc[0, sr, at, :] = jnp.broadcast_to(turned[:, c : c + 1], (TILE, TILE))
            sc[1, sr, at, :] = jnp.broadcast_to(turned[:, GX + c : GX + c + 1], (TILE, TILE))

    for side, sr in ((0, 0), (1, rows + 1)):
        @pl.when(jnp.logical_not(has[side]))
        def _(sr=sr):
            sc[0, sr] = jnp.full((sc.shape[2], TILE), FAR, F32)
            sc[1, sr] = jnp.full((sc.shape[2], TILE), FAR, F32)

    def split(par, sr, at, value):
        high = value.astype(BF16)
        vx[par, sr, 0:PAD, at] = high
        vx[par, sr, PAD : 2 * PAD, at] = (value - high.astype(F32)).astype(BF16)

    own = pl.ds(TILE, row_lanes)
    for a in range(rows):
        base = a * row_lanes
        split(0, a + 1, own, pk[0, :, base : base + row_lanes])
        place_columns(
            a + 1,
            [
                (
                    (pk[0, RHS : RHS + 1, base + c * TILE : base + (c + 1) * TILE] + a) * inverse,
                    (pk[0, RHS + 1 : RHS + 2, base + c * TILE : base + (c + 1) * TILE] + c) * inverse,
                )
                for c in range(GX)
            ],
        )

    def build(high_ref, low_ref, a, c, sr, first):
        base = pl.multiple_of(a * row_lanes + c * TILE, TILE)
        here = pk[0, :, pl.ds(base, TILE)]
        tx = (here[RHS : RHS + 1] + a) * inverse
        ty = (here[RHS + 1 : RHS + 2] + c.astype(F32)) * inverse
        step = 64
        for part in range(reach // step):
            at = pl.ds(pl.multiple_of(c * TILE + part * step, step), step)
            dx = sc[0, sr, at, :] - tx
            dy = sc[1, sr, at, :] - ty
            square = dx * dx + dy * dy
            close = jnp.maximum(1.0 - square * lax.rsqrt(jnp.maximum(square, TINY)), 0.0)
            twice = close * close
            w = twice * twice * (5.0 - 4.0 * close)
            high = w.astype(BF16)
            to = pl.ds(first + part * step, step)
            high_ref[to, :] = high
            low_ref[to, :] = (w - high.astype(F32)).astype(BF16)

    def apply(v, high_ref, low_ref):
        high, low = (
            jnp.concatenate([held[t] for t in range(held.shape[0])], axis=1)
            for held in (high_ref, low_ref)
        )
        r = jnp.dot(v, high, preferred_element_type=F32)
        s = jnp.dot(v[:PAD], low, preferred_element_type=F32)
        return r[:PAD] + r[PAD:] + s

    pair = 2 * TILE
    zero = jnp.zeros((PAD, TILE), F32)
    moments = []
    for k in range(3):
        par = k % 2

        def inner(c, carry, k=k, par=par):
            if k == 0:
                for sr in range(1, rows + 1):
                    for a in range(rows):
                        build(whi.at[c, a], wlo.at[c, a], a, c, sr, (sr - 1) * reach)
            lanes = pl.ds(pl.multiple_of(c * TILE, TILE), reach)
            v = jnp.concatenate([vx[par, sr, :, lanes] for sr in range(1, rows + 1)], axis=1)
            part = apply(v, whi.at[c], wlo.at[c])
            for a in range(rows):
                at = pl.ds(pl.multiple_of(a * row_lanes + c * TILE, TILE), TILE)
                acc[:, at] = part[:, a * TILE : (a + 1) * TILE]
            return carry

        lax.fori_loop(0, GX, inner, 0, unroll=2 if k == 0 else 8)

        for side, sr in ((0, 0), (1, rows + 1)):
            @pl.when(has[side])
            def _(side=side, sr=sr, k=k, par=par):
                pltpu.make_async_remote_copy(
                    src_ref=pk.at[k, :, pl.ds(0, row_lanes)],
                    dst_ref=hv.at[k, side],
                    send_sem=halo_send.at[k, side],
                    recv_sem=halo_recv.at[k, side],
                    device_id={"rows": me - 1 if side == 0 else me + 1},
                    device_id_type=MESH,
                ).wait_recv()
                split(par, sr, own, hv[k, side])
                if k == 0:
                    place_columns(
                        sr,
                        [
                            (
                                (hv[0, side, RHS : RHS + 1, c * TILE : (c + 1) * TILE] + (sr - 1)) * inverse,
                                (hv[0, side, RHS + 1 : RHS + 2, c * TILE : (c + 1) * TILE] + c) * inverse,
                            )
                            for c in range(GX)
                        ],
                    )

        def outer(c, carry, k=k, par=par):
            first, cross, square = carry
            sources = pl.ds(pl.multiple_of(c * pair, pair), 2 * pair)
            for a in range(rows):
                at = pl.ds(pl.multiple_of(a * row_lanes + c * pair, pair), pair)
                total = acc[:, at]
                for side, sr, edge in ((0, 0, 0), (1, rows + 1, rows - 1)):
                    if a != edge:
                        continue
                    if k == 0:
                        for held in (ohi, olo):
                            held[side, c, 0, 3 * TILE :] = jnp.zeros((TILE, TILE), BF16)
                            held[side, c, 1, :TILE] = jnp.zeros((TILE, TILE), BF16)
                        for t in range(2):
                            build(
                                ohi.at[side, c, t], olo.at[side, c, t], a, 2 * c + t, sr, t * TILE
                            )
                    total = total + apply(
                        vx[par, sr, :, sources], ohi.at[side, c], olo.at[side, c]
                    )
                now = pk[k, :, at]
                later = amp * (total - now)
                if k == 0:
                    first = first + now * now
                cross = cross + now * later
                if k < 2:
                    square = square + later * later
                    pk[k + 1, :, at] = later
                    split(1 - par, a + 1, pl.ds(pl.multiple_of(c * pair + TILE, TILE), pair), later)
            return first, cross, square

        wide = jnp.zeros((PAD, pair), F32)
        first, cross, square = lax.fori_loop(0, GX // 2, outer, (wide, wide, wide), unroll=1 if k == 0 else 8)
        moments += ([first] if k == 0 else []) + [cross] + ([square] if k < 2 else [])
        if k < 2:
            send_halo(k + 1)

    lane = lax.broadcasted_iota(jnp.int32, (PAD, TILE), 1)
    packed = zero
    for i, part in enumerate(moments):
        packed = jnp.where(lane == i, jnp.sum(part, axis=1, keepdims=True), packed)
    mom[...] = packed
    gathered[me] = packed

    def mom_copy(k):
        peer = lax.rem(me + k, n)
        return pltpu.make_async_remote_copy(
            src_ref=mom,
            dst_ref=gathered.at[me],
            send_sem=mom_send.at[peer],
            recv_sem=mom_recv.at[me],
            device_id={"rows": peer},
            device_id_type=MESH,
        )

    def mom_start(k, carry):
        mom_copy(k).start()
        return carry

    lax.fori_loop(1, n, mom_start, 0)

    def mom_wait(k, carry):
        peer = lax.rem(me + k, n)
        pltpu.make_async_remote_copy(
            src_ref=mom,
            dst_ref=gathered.at[peer],
            send_sem=mom_send.at[peer],
            recv_sem=mom_recv.at[peer],
            device_id={"rows": peer},
            device_id_type=MESH,
        ).wait()
        return carry

    lax.fori_loop(1, n, mom_wait, 0)
    total = lax.fori_loop(0, n, lambda j, t: t + gathered[j], zero)

    m = [total[:, i : i + 1] for i in range(6)]
    a00, a01, a02 = (m[i + 1] + shift * m[i] for i in range(3))
    a11, a12 = (m[i + 1] + shift * m[i] for i in range(2, 4))
    a22 = m[5] + shift * m[4]
    l1 = a01 / a00
    l2 = a02 / a00
    b11 = a11 - l1 * a01
    b12 = a12 - l1 * a02
    b22 = a22 - l2 * a02
    g1 = m[1] - l1 * m[0]
    g2 = m[2] - l2 * m[0]
    fine1 = b11 > 1.0e-6 * a11
    safe1 = jnp.where(fine1, b11, 1.0)
    l3 = b12 / safe1
    d22 = b22 - l3 * b12
    fine2 = jnp.logical_and(fine1, d22 > 1.0e-6 * a22)
    c2 = jnp.where(fine2, (g2 - l3 * g1) / jnp.where(fine2, d22, 1.0), 0.0)
    c1 = jnp.where(fine1, (g1 - b12 * c2) / safe1, 0.0)
    c0 = (m[0] - a01 * c1 - a02 * c2) / a00
    values = (c0 * m[0] + c1 * m[1] + c2 * m[2]) / points
    sublane = lax.broadcasted_iota(jnp.int32, (PAD, TILE), 0)
    turned = jnp.sum(jnp.where(lane == sublane, values, 0.0), axis=0, keepdims=True)
    q_ref[...] = turned[:, :RHS]

    for g in range(rows * GX):
        at = slice(g * TILE, (g + 1) * TILE)
        tiles[g] = c0 * pk[0, :, at] + c1 * pk[1, :, at] + c2 * pk[2, :, at]
    for s in range(rows * GX):
        found = tiles[cell[s]]
        x_ref[:, s * TILE : (s + 1) * TILE] = found[:RHS]

    for k in range(3):
        for side in range(2):
            @pl.when(has[side])
            def _(k=k, side=side):
                halo_copy(k, side).wait_send()


def shards(n, offsets, tile_cell, probes, target, lengthscale, amplitude, noise):
    tiles = tile_cell.shape[0]
    rows = tiles // GX
    places = jnp.arange(tiles, dtype=jnp.int32)
    order = jnp.sum(
        jnp.where(tile_cell[None, :] == places[:, None], places[None, :], 0), axis=1
    ).astype(jnp.int32)
    local = tiles * TILE
    width = (GX + 2) * TILE
    smem = pl.BlockSpec(memory_space=pltpu.SMEM)
    vmem = pl.BlockSpec(memory_space=pltpu.VMEM)
    solutions, quadratic = pl.pallas_call(
        functools.partial(kernel, n, rows, float(local * n)),
        out_shape=(
            jax.ShapeDtypeStruct((RHS, local), F32),
            jax.ShapeDtypeStruct((1, RHS), F32),
        ),
        in_specs=[smem] * 5 + [pl.BlockSpec(memory_space=pl.ANY)] * 3,
        out_specs=(vmem, vmem),
        scratch_shapes=[
            pltpu.VMEM((2, local), F32),
            pltpu.VMEM((RHS - 1, local), jnp.int32),
            pltpu.VMEM((1, local), F32),
            pltpu.VMEM((tiles, PAD, TILE), F32),
            pltpu.VMEM((3, PAD, local), F32),
            pltpu.VMEM((3, 2, PAD, GX * TILE), F32),
            pltpu.VMEM((2, rows + 2, 2 * PAD, width), BF16),
            pltpu.VMEM((GX, rows, rows * 3 * TILE, TILE), BF16),
            pltpu.VMEM((GX, rows, rows * 3 * TILE, TILE), BF16),
            pltpu.VMEM((2, GX // 2, 2, 4 * TILE, TILE), BF16),
            pltpu.VMEM((2, GX // 2, 2, 4 * TILE, TILE), BF16),
            pltpu.VMEM((2, rows + 2, width, TILE), F32),
            pltpu.VMEM((TILE, TILE), F32),
            pltpu.VMEM((PAD, local), F32),
            pltpu.VMEM((PAD, TILE), F32),
            pltpu.VMEM((n, PAD, TILE), F32),
            pltpu.SemaphoreType.DMA((3,)),
            pltpu.SemaphoreType.DMA((3, 2)),
            pltpu.SemaphoreType.DMA((3, 2)),
            pltpu.SemaphoreType.DMA((n,)),
            pltpu.SemaphoreType.DMA((n,)),
        ],
        compiler_params=pltpu.CompilerParams(
            collective_id=0, has_side_effects=True, vmem_limit_bytes=58 * 1024 * 1024
        ),
        name="solve",
    )(order, tile_cell, lengthscale, amplitude, noise, offsets, probes, target[None, :])
    return solutions, quadratic.reshape(RHS)


def solution(mesh):
    return jax.shard_map(
        functools.partial(shards, mesh.shape["rows"]),
        mesh=mesh,
        in_specs=(
            P(None, "rows"),
            P("rows"),
            P(None, "rows"),
            P("rows"),
            P("hyp"),
            P("hyp"),
            P("hyp"),
        ),
        out_specs=(P("hyp", "rows"), P("hyp")),
        check_vma=False,
    )
```
